32 devices in a mesh: ma: 16 (over z, x, core), dev: 2 (over y).
Axes of the slice: x: 2, y: 2, z: 4, core: 2. Of those that a mesh axis runs over, the one named last changes fastest.
Arguments:
- grid_latent: bfloat16 [16384, 512], P('ma'), may hold values from -6 to 6
- mesh_latent: bfloat16 [10240, 512], P('ma'), may hold values from -6 to 6
- grid_map: int32 [10240, 4], P('ma'), may hold values from 0 to 16383, as said below
- fine_senders: int32 [10240, 6], P('ma'), may hold values from 0 to 10239, as said below
- coarse_senders: int32 [256, 24], P('ma'), may hold values from 0 to 255
- fine_geom: float32 [10240, 6, 4], P('ma'), may hold values from -6 to 6
- coarse_geom: float32 [256, 24, 4], P('ma'), may hold values from -6 to 6
- w_send: bfloat16 [2, 512, 512], P(None, None, 'dev'), may hold values from -0.1875 to 0.1875
- w_recv: bfloat16 [2, 512, 512], P(None, None, 'dev'), may hold values from -0.1875 to 0.1875
- w_geom: float32 [2, 4, 512], P(None, None, 'dev'), may hold values from -2 to 2
- edge_bias: float32 [2, 512], P(None, 'dev'), may hold values from -3 to 3
- w_msg: bfloat16 [2, 512, 512], P(None, 'dev'), may hold values from -0.25 to 0.25
- msg_bias: float32 [2, 512], replicated, may hold values from -2 to 2
- w_node_h: bfloat16 [2, 512, 512], P(None, None, 'dev'), may hold values from -0.1875 to 0.1875
- w_node_a: bfloat16 [2, 512, 512], P(None, None, 'dev'), may hold values from -0.125 to 0.125
- node_bias: float32 [2, 512], P(None, 'dev'), may hold values from -3 to 3
- w_node_out: bfloat16 [2, 512, 512], P(None, 'dev'), may hold values from -0.25 to 0.25
- norm_gain: float32 [2, 512], replicated, may hold values from 0.25 to 1.75
- norm_bias: float32 [2, 512], replicated, may hold values from -2 to 2
Outputs:
- new_latent: bfloat16 [10240, 512], P('ma')
The draws below stay inside these ranges and needn't reach their ends.
Inputs may be any that keep to these rules, and one draw needn't show every extreme that they name: For a node n in patch p = n // 640, every grid_map[n, k] equals (p * 1024 + o) modulo 16384 with -512 <= o < 1536; both ends of that band are used in every patch. For a node n in patch p = n // 640, every fine_senders[n, j] equals (p * 640 + o) modulo 10240 with -320 <= o < 960; both ends of that band are used in every patch. `coarse_senders`: any coarse node may send to any coarse node.
All inputs are finite; a program needn't handle non-finite values.
Results may differ from the reference program's by a relative error of at most 0.015.
Values may be sent and summed in bfloat16 or wider, within the bound.
A program may use at most 64 MiB of HBM per device.

```python
import jax
import jax.numpy as jnp
from jax import lax

D = 512
NODE_DEV = 640
GRID_DEV = 1024
CO_DEV = 16
FINE_IN = 6
COARSE_IN = 24
G2M_K = 4
GEO = 4
PASSES = 2
NODE_EDGE = 320
GRID_EDGE = 512
NODES = 10240
GRID = 16384
COARSE = 256


def banded(key, rows_each, cols, span, border, total):
    patches = total // span
    offsets = jax.random.randint(key, (patches, rows_each, cols), -border, span + border)
    offsets = offsets.at[:, 0, 0].set(-border)
    offsets = offsets.at[:, rows_each - 1, 0].set(span + border - 1)
    anchor = (jnp.arange(patches, dtype=jnp.int32) * span)[:, None, None]
    return ((anchor + offsets) % total).reshape(patches * rows_each, cols).astype(jnp.int32)


def draw_grid_map(key, part):
    return banded(jax.random.fold_in(key, 11), NODE_DEV, G2M_K, GRID_DEV, GRID_EDGE, GRID)


def draw_fine_senders(key, part):
    return banded(jax.random.fold_in(key, 23), NODE_DEV, FINE_IN, NODE_DEV, NODE_EDGE, NODES)


def place_ends(result, key, smallest, largest):
    place = [jax.random.randint(jax.random.fold_in(key, axis), (), 0, length) for axis, length in enumerate(result.shape)]
    widest = result.shape.index(max(result.shape))
    beside = place[:widest] + [(place[widest] + 1) % result.shape[widest]] + place[widest + 1:]
    return result.at[tuple(place)].set(smallest).at[tuple(beside)].set(largest)


def levels(stream_key, dims, shards, least, high):
    factor_of, own = 1.0, jax.random.fold_in(stream_key, 6)
    for position, blocks in shards:
        heights = jnp.exp(jax.random.uniform(jax.random.fold_in(own, position), (blocks,), jnp.float32, least / len(shards), high / len(shards)))
        factor_of = factor_of * jnp.repeat(heights, dims[position] // blocks).reshape([-1 if axis == position else 1 for axis in range(len(dims))])
    return factor_of


def normal_values(rng, dims, scale, most, split=(), held_as=jnp.bfloat16):
    array = scale * jax.random.normal(rng, dims, jnp.float32)
    if split:
        array = array * levels(rng, dims, split, -0.22, 0.18)
    return jnp.clip(array, -most, most).astype(held_as)


def setup_inputs(seed: int = 0) -> dict:
    key_of = jax.random.split(jax.random.key(seed), 20)
    grid_latent = normal_values(key_of[0], (GRID, D), 1.0, 6.0, ((0, 16),))
    mesh_latent = normal_values(key_of[1], (NODES, D), 1.0, 6.0, ((0, 16),))
    grid_map = draw_grid_map(jax.random.fold_in(key_of[19], 71), 0)
    fine_senders = draw_fine_senders(jax.random.fold_in(key_of[19], 71), 0)
    coarse_senders = place_ends(jax.random.randint(key_of[4], (COARSE, COARSE_IN), 0, COARSE), jax.random.fold_in(key_of[4], 1), 0, COARSE - 1).astype(jnp.int32)
    fine_geom = normal_values(key_of[5], (NODES, FINE_IN, GEO), 1.0, 6.0, ((0, 16),), jnp.float32)
    coarse_geom = normal_values(key_of[6], (COARSE, COARSE_IN, GEO), 1.0, 6.0, ((0, 16),), jnp.float32)
    w_send = normal_values(key_of[7], (PASSES, D, D), (2 * D) ** -0.5, 0.1875, ((2, 2),))
    w_recv = normal_values(key_of[8], (PASSES, D, D), (2 * D) ** -0.5, 0.1875, ((2, 2),))
    w_geom = normal_values(key_of[9], (PASSES, GEO, D), (2 * GEO) ** -0.5, 2.0, ((2, 2),), jnp.float32)
    edge_bias = normal_values(key_of[10], (PASSES, D), 0.5, 3.0, ((1, 2),), jnp.float32)
    w_msg = normal_values(key_of[11], (PASSES, D, D), D ** -0.5, 0.25, ((1, 2),))
    msg_bias = normal_values(key_of[12], (PASSES, D), 0.3, 2.0, (), jnp.float32)
    w_node_h = normal_values(key_of[13], (PASSES, D, D), (2 * D) ** -0.5, 0.1875, ((2, 2),))
    w_node_a = normal_values(key_of[14], (PASSES, D, D), (4 * D) ** -0.5, 0.125, ((2, 2),))
    node_bias = normal_values(key_of[15], (PASSES, D), 0.5, 3.0, ((1, 2),), jnp.float32)
    w_node_out = normal_values(key_of[16], (PASSES, D, D), D ** -0.5, 0.25, ((1, 2),))
    norm_gain = jnp.clip(1.0 + 0.15 * jax.random.normal(key_of[17], (PASSES, D), jnp.float32), 0.25, 1.75)
    norm_bias = normal_values(key_of[18], (PASSES, D), 0.3, 2.0, (), jnp.float32)
    return {"grid_latent": grid_latent, "mesh_latent": mesh_latent, "grid_map": grid_map, "fine_senders": fine_senders, "coarse_senders": coarse_senders, "fine_geom": fine_geom, "coarse_geom": coarse_geom, "w_send": w_send, "w_recv": w_recv, "w_geom": w_geom, "edge_bias": edge_bias, "w_msg": w_msg, "msg_bias": msg_bias, "w_node_h": w_node_h, "w_node_a": w_node_a, "node_bias": node_bias, "w_node_out": w_node_out, "norm_gain": norm_gain, "norm_bias": norm_bias}


norm_eps = 1e-05

def reference(grid_latent, mesh_latent, grid_map, fine_senders, coarse_senders, fine_geom, coarse_geom, w_send, w_recv, w_geom, edge_bias, w_msg, msg_bias, w_node_h, w_node_a, node_bias, w_node_out, norm_gain, norm_bias):
    pulled = jnp.take(grid_latent, grid_map, axis=0).astype(jnp.float32)
    latent = (mesh_latent.astype(jnp.float32) + lax.optimization_barrier(jnp.mean(pulled, axis=1))).astype(jnp.bfloat16)
    coarse_ids = jnp.arange(COARSE, dtype=jnp.int32)
    coarse_rows = (coarse_ids // CO_DEV * NODE_DEV + coarse_ids % CO_DEV).astype(jnp.int32)
    for pass_idx in range(PASSES):
        send_proj = jnp.dot(latent, w_send[pass_idx], preferred_element_type=jnp.float32).astype(jnp.bfloat16)
        recv_proj = jnp.dot(latent, w_recv[pass_idx], preferred_element_type=jnp.float32).astype(jnp.bfloat16)
        fine_geo = jnp.einsum('nkg,gd->nkd', fine_geom, w_geom[pass_idx], precision=lax.Precision.HIGHEST)
        fine_pre = send_proj[fine_senders].astype(jnp.float32) + recv_proj[:, None, :].astype(jnp.float32) + fine_geo + edge_bias[pass_idx]
        fine_hidden = jax.nn.silu(fine_pre).astype(jnp.bfloat16).reshape(NODES * FINE_IN, D)
        fine_msg = jnp.dot(fine_hidden, w_msg[pass_idx], preferred_element_type=jnp.float32) + msg_bias[pass_idx]
        fine_sum = lax.optimization_barrier(jnp.sum(fine_msg.reshape(NODES, FINE_IN, D), axis=1))
        coarse_send = send_proj[coarse_rows]
        coarse_recv = recv_proj[coarse_rows]
        coarse_geo = jnp.einsum('nkg,gd->nkd', coarse_geom, w_geom[pass_idx], precision=lax.Precision.HIGHEST)
        coarse_pre = coarse_send[coarse_senders].astype(jnp.float32) + coarse_recv[:, None, :].astype(jnp.float32) + coarse_geo + edge_bias[pass_idx]
        coarse_hidden = jax.nn.silu(coarse_pre).astype(jnp.bfloat16).reshape(COARSE * COARSE_IN, D)
        coarse_msg = jnp.dot(coarse_hidden, w_msg[pass_idx], preferred_element_type=jnp.float32) + msg_bias[pass_idx]
        coarse_sum = lax.optimization_barrier(jnp.sum(coarse_msg.reshape(COARSE, COARSE_IN, D), axis=1))
        agg = fine_sum.at[coarse_rows].add(coarse_sum).astype(jnp.bfloat16)
        node_pre = jnp.dot(latent, w_node_h[pass_idx], preferred_element_type=jnp.float32) + jnp.dot(agg, w_node_a[pass_idx], preferred_element_type=jnp.float32) + node_bias[pass_idx]
        node_hidden = jax.nn.silu(node_pre).astype(jnp.bfloat16)
        update = jnp.dot(node_hidden, w_node_out[pass_idx], preferred_element_type=jnp.float32)
        average = lax.optimization_barrier(jnp.mean(update, axis=1, keepdims=True))
        spread = lax.optimization_barrier(jnp.mean(update * update, axis=1, keepdims=True)) - average * average
        normed = (update - average) * lax.rsqrt(spread + norm_eps) * norm_gain[pass_idx] + norm_bias[pass_idx]
        latent = (latent.astype(jnp.float32) + normed).astype(jnp.bfloat16)
    return latent
```

```python
import functools

import jax
import jax.numpy as jnp
from jax import lax
from jax.experimental import pallas as pl
from jax.experimental.pallas import tpu as pltpu
from jax.sharding import PartitionSpec as P

norm_eps = 1e-05
MESH = pl.DeviceIdType.MESH
slot_w = 8


def round_up(value, step):
    return (value + step - 1) // step * step


def silu(x):
    half = 0.5 * x
    return half + half * jnp.tanh(half)


def split_two(x):
    high = x.astype(jnp.bfloat16)
    low = (x - high.astype(jnp.float32)).astype(jnp.bfloat16)
    return high, low


def wrapped(index, base, total):
    v = index - base
    v = jnp.where(v < 0, v + total, v)
    return jnp.where(v >= total, v - total, v)


def kernel(
    patches,
    geo_terms,
    grid_ref,
    mesh_ref,
    map_ref,
    fine_ref,
    cidx_ref,
    fgeo_ref,
    cgeo_ref,
    prm_ref,
    ws_ref,
    wr_ref,
    wh_ref,
    wa_ref,
    wm_ref,
    wo_ref,
    mbias_ref,
    gain_ref,
    nbias_ref,
    out_ref,
    gpad,
    cmat,
    oh,
    coh,
    spad,
    ever,
    recv,
    lat,
    hsum,
    nhid,
    wc,
    wrow,
    prm,
    loc_sem,
    gs_sem,
    gr_sem,
    ys_sem,
    yr_sem,
    fs_sem,
    fr_sem,
    ps_sem,
    hs_sem,
    hr_sem,
    cs_sem,
    cr_sem,
):
    me = lax.axis_index("ma")
    dev = lax.axis_index("dev")
    other = 1 - dev
    core = lax.rem(me, 2)
    sibling = me + 1 - 2 * core
    right = lax.rem(me + 1, patches)
    left = lax.rem(me + patches - 1, patches)
    grid_dev = grid_ref.shape[0]
    node_dev, features = mesh_ref.shape
    layers = ws_ref.shape[0]
    fine_in = fine_ref.shape[1]
    half = ws_ref.shape[2]
    gb, nb = grid_dev // 2, node_dev // 2
    span = 2 * node_dev
    co_edges = cidx_ref.shape[0]
    coarse = ever.shape[1] - cgeo_ref.shape[1]
    co_dev = coarse // patches
    coarse_in = co_edges // co_dev
    blk = 128
    nblk = node_dev // blk

    barrier = pltpu.get_barrier_semaphore()

    def greet(step, _):
        peer = lax.rem(me + step, patches)
        pl.semaphore_signal(barrier, inc=1, device_id={"ma": peer}, device_id_type=MESH)
        return 0

    lax.fori_loop(1, patches, greet, 0)
    pl.semaphore_signal(barrier, inc=1, device_id={"dev": other}, device_id_type=MESH)
    pl.semaphore_wait(barrier, patches)

    to_left = pltpu.make_async_remote_copy(
        src_ref=grid_ref.at[pl.ds(0, gb)],
        dst_ref=gpad.at[pl.ds(gb + grid_dev, gb)],
        send_sem=gs_sem.at[0],
        recv_sem=gr_sem.at[0],
        device_id={"ma": left},
        device_id_type=MESH,
    )
    to_right = pltpu.make_async_remote_copy(
        src_ref=grid_ref.at[pl.ds(grid_dev - gb, gb)],
        dst_ref=gpad.at[pl.ds(0, gb)],
        send_sem=gs_sem.at[1],
        recv_sem=gr_sem.at[1],
        device_id={"ma": right},
        device_id_type=MESH,
    )
    to_left.start()
    to_right.start()
    grid_own = pltpu.make_async_copy(grid_ref, gpad.at[pl.ds(gb, grid_dev)], loc_sem.at[layers, 0])
    grid_own.start()

    prm_out = pltpu.make_async_remote_copy(
        src_ref=prm_ref,
        dst_ref=prm.at[dev],
        send_sem=ps_sem.at[0],
        recv_sem=ps_sem.at[1],
        device_id={"dev": other},
        device_id_type=MESH,
    )
    prm_out.start()
    prm_own = pltpu.make_async_copy(prm_ref, prm.at[dev], loc_sem.at[layers, 1])
    prm_own.start()
    cols = (ws_ref, wr_ref, wh_ref, wa_ref)
    rows = (wm_ref, wo_ref)
    order = (0, 1, 4, 2, 3, 5)

    def own_part(layer, i):
        if i < 4:
            n = features // 2
            return cols[i].at[layer, pl.ds(core * n, n), :]
        n = half // 2
        return rows[i - 4].at[layer, pl.ds(core * n, n), :]

    def slot(layer, i, side, part):
        if i < 4:
            n = features // 2
            return wc.at[layer, i, side, pl.ds(part * n, n), :]
        n = half // 2
        return wrow.at[layer, i - 4, pl.ds(side * half + part * n, n), :]

    def y_copy(layer, i):
        return pltpu.make_async_remote_copy(
            src_ref=own_part(layer, i),
            dst_ref=slot(layer, i, dev, core),
            send_sem=ys_sem.at[layer, i],
            recv_sem=yr_sem.at[layer, i],
            device_id={"dev": other},
            device_id_type=MESH,
        )

    def y_wait(layer, i):
        got = slot(layer, i, other, core)
        pltpu.make_async_remote_copy(
            src_ref=got,
            dst_ref=got,
            send_sem=ys_sem.at[layer, i],
            recv_sem=yr_sem.at[layer, i],
            device_id={"dev": other},
            device_id_type=MESH,
        ).wait_recv()

    def f_copy(layer, i, part):
        got = slot(layer, i, other, part)
        return pltpu.make_async_remote_copy(
            src_ref=got,
            dst_ref=got,
            send_sem=fs_sem.at[layer, i],
            recv_sem=fr_sem.at[layer, i],
            device_id={"ma": sibling},
            device_id_type=MESH,
        )

    def local_copy(layer, i):
        if i < 4:
            return pltpu.make_async_copy(
                cols[i].at[layer], wc.at[layer, i, dev], loc_sem.at[layer, i]
            )
        return pltpu.make_async_copy(
            rows[i - 4].at[layer],
            wrow.at[layer, i - 4, pl.ds(dev * half, half), :],
            loc_sem.at[layer, i],
        )

    for layer in range(layers):
        for i in order:
            y_copy(layer, i).start()
    for layer in range(layers):
        for i in order:
            local_copy(layer, i).start()

    def forward(layer, i):
        y_wait(layer, i)
        f_copy(layer, i, core).start()

    def ready(layer, i):
        local_copy(layer, i).wait()
        f_copy(layer, i, 1 - core).wait_recv()

    ext = fgeo_ref.shape[1]
    base = me * node_dev - nb
    gbase = me * grid_dev - gb

    def counts(b, _):
        r = pl.ds(b * blk, blk)
        idx = wrapped(map_ref[r, :], gbase, grid_dev * patches)
        lanes = lax.broadcasted_iota(jnp.int32, (blk, 2 * grid_dev), 1)
        total = jnp.zeros((blk, 2 * grid_dev), jnp.float32)
        for k in range(map_ref.shape[1]):
            total = total + jnp.where(lanes == idx[:, k : k + 1], 1.0, 0.0)
        cmat[r, :] = total.astype(jnp.bfloat16)
        return 0

    lax.fori_loop(0, nblk, counts, 0)

    glane = lax.broadcasted_iota(jnp.int32, (blk, ext), 1)
    gterm = fine_in * slot_w

    def one_hots(b, _):
        r = pl.ds(b * blk, blk)
        idx = wrapped(fine_ref[r, :], base, node_dev * patches)
        lanes = lax.broadcasted_iota(jnp.int32, (blk, span), 1)
        high, low = split_two(fgeo_ref[r, :])
        both = jnp.where(glane < 2 * gterm, high.astype(jnp.float32), low.astype(jnp.float32))
        which = lax.rem(lax.div(glane, slot_w), fine_in)
        for j in range(fine_in):
            oh[j, r, :span] = jnp.where(lanes == idx[:, j : j + 1], 1.0, 0.0).astype(jnp.bfloat16)
            oh[j, r, span:] = jnp.where(which == j, both, 0.0).astype(jnp.bfloat16)
        return 0

    lax.fori_loop(0, nblk, one_hots, 0)

    clanes = lax.broadcasted_iota(jnp.int32, (co_edges, coarse), 1)
    coh[:, :coarse] = jnp.where(clanes == cidx_ref[...], 1.0, 0.0).astype(jnp.bfloat16)
    cext = cgeo_ref.shape[1]
    high, low = split_two(cgeo_ref[...])
    clane = lax.broadcasted_iota(jnp.int32, (co_edges, cext), 1)
    coh[:, coarse:] = jnp.where(
        clane < 2 * slot_w, high.astype(jnp.float32), low.astype(jnp.float32)
    ).astype(jnp.bfloat16)

    prm_own.wait()
    prm_in = pltpu.make_async_remote_copy(
        src_ref=prm.at[other],
        dst_ref=prm.at[other],
        send_sem=ps_sem.at[0],
        recv_sem=ps_sem.at[1],
        device_id={"dev": other},
        device_id_type=MESH,
    )
    prm_in.wait_recv()
    for layer in range(layers):
        for side in range(2):
            c = pl.ds(side * half, half)
            high, low = split_two(prm[side, layer])
            high, low = high.astype(jnp.float32), low.astype(jnp.float32)
            pad = ext - geo_terms * gterm
            pieces = [high] * fine_in + [low] * fine_in + [high] * fine_in
            if pad:
                pieces.append(jnp.zeros((pad, half), jnp.float32))
            spad[layer, span:, c] = jnp.concatenate(pieces, axis=0).astype(jnp.bfloat16)
            pieces = [high, low, high]
            pieces.append(jnp.zeros((cext - geo_terms * slot_w, half), jnp.float32))
            ever[layer, coarse:, c] = jnp.concatenate(pieces, axis=0).astype(jnp.bfloat16)

    for i in (0, 1):
        forward(0, i)
    grid_own.wait()
    to_left.wait_recv()
    to_right.wait_recv()

    def encode(b, _):
        r = pl.ds(b * blk, blk)
        mean = jnp.dot(cmat[r, :], gpad[...], preferred_element_type=jnp.float32)
        mean = mean * (1.0 / map_ref.shape[1])
        lat[r, :] = (mesh_ref[r, :].astype(jnp.float32) + mean).astype(jnp.bfloat16)
        return 0

    lax.fori_loop(0, nblk, encode, 0)

    for layer in range(layers):
        ready(layer, 0)

        def project_send(b, _):
            r = pl.ds(b * blk, blk)
            x = lat[r, :]
            for side in range(2):
                spad[layer, pl.ds(nb + b * blk, blk), side * half : (side + 1) * half] = jnp.dot(
                    x, wc[layer, 0, side], preferred_element_type=jnp.float32
                ).astype(jnp.bfloat16)
            return 0

        lax.fori_loop(0, nblk, project_send, 0)

        halo_left = pltpu.make_async_remote_copy(
            src_ref=spad.at[layer, pl.ds(nb, nb), :],
            dst_ref=spad.at[layer, pl.ds(nb + node_dev, nb), :],
            send_sem=hs_sem.at[layer, 0],
            recv_sem=hr_sem.at[layer, 0],
            device_id={"ma": left},
            device_id_type=MESH,
        )
        halo_right = pltpu.make_async_remote_copy(
            src_ref=spad.at[layer, pl.ds(node_dev, nb), :],
            dst_ref=spad.at[layer, pl.ds(0, nb), :],
            send_sem=hs_sem.at[layer, 1],
            recv_sem=hr_sem.at[layer, 1],
            device_id={"ma": right},
            device_id_type=MESH,
        )
        halo_left.start()
        halo_right.start()

        def coarse_copy(step):
            peer = lax.rem(me + step, patches)
            return pltpu.make_async_remote_copy(
                src_ref=spad.at[layer, pl.ds(nb, co_dev), :],
                dst_ref=ever.at[layer, pl.ds(me * co_dev, co_dev), :],
                send_sem=cs_sem.at[layer, step],
                recv_sem=cr_sem.at[layer, step],
                device_id={"ma": peer},
                device_id_type=MESH,
            )

        def coarse_start(step, _):
            coarse_copy(step).start()
            return 0

        lax.fori_loop(1, patches, coarse_start, 0)
        ever[layer, pl.ds(pl.multiple_of(me * co_dev, co_dev), co_dev), :] = spad[
            layer, nb : nb + co_dev, :
        ]

        ready(layer, 1)

        def project_recv(b, _):
            r = pl.ds(b * blk, blk)
            x = lat[r, :]
            for side in range(2):
                recv[r, side * half : (side + 1) * half] = jnp.dot(
                    x, wc[layer, 1, side], preferred_element_type=jnp.float32
                ).astype(jnp.bfloat16)
            return 0

        lax.fori_loop(0, nblk, project_recv, 0)
        for i in (4, 2, 3, 5):
            if layer == 0:
                forward(0, i)

        halo_left.wait_recv()
        halo_right.wait_recv()

        def edges(b, _):
            r = pl.ds(b * blk, blk)
            x = recv[r, :].astype(jnp.float32)
            total = jnp.zeros((blk, features), jnp.float32)
            for j in range(fine_in):
                pre = jnp.dot(oh[j, r, :], spad[layer], preferred_element_type=jnp.float32)
                total = total + silu(pre + x)
            hsum[r, :] = total
            return 0

        lax.fori_loop(0, nblk, edges, 0)

        def coarse_wait(step, _):
            source = lax.rem(me + patches - step, patches)
            got = ever.at[layer, pl.ds(source * co_dev, co_dev), :]
            pltpu.make_async_remote_copy(
                src_ref=got,
                dst_ref=got,
                send_sem=cs_sem.at[layer, step],
                recv_sem=cr_sem.at[layer, step],
                device_id={"ma": source},
                device_id_type=MESH,
            ).wait_recv()
            return 0

        lax.fori_loop(1, patches, coarse_wait, 0)
        cpre = jnp.dot(coh[...], ever[layer], preferred_element_type=jnp.float32)
        x = recv[:co_dev, :].astype(jnp.float32)
        total = hsum[:co_dev, :]
        for j in range(coarse_in):
            total = total + silu(cpre[j * co_dev : (j + 1) * co_dev, :] + x)
        hsum[:co_dev, :] = total

        if layer + 1 < layers:
            for i in order:
                forward(layer + 1, i)
        for i in (4, 2, 3, 5):
            ready(layer, i)

        def nodes(b, _):
            r = pl.ds(b * blk, blk)
            agg = jnp.dot(
                hsum[r, :].astype(jnp.bfloat16), wrow[layer, 0], preferred_element_type=jnp.float32
            )
            position = b * blk + lax.broadcasted_iota(jnp.int32, (blk, features), 0)
            count = jnp.where(position < co_dev, float(fine_in + coarse_in), float(fine_in))
            agg = (agg + count * mbias_ref[layer : layer + 1, :]).astype(jnp.bfloat16)
            x = lat[r, :]
            for side in range(2):
                pre = (
                    jnp.dot(x, wc[layer, 2, side], preferred_element_type=jnp.float32)
                    + jnp.dot(agg, wc[layer, 3, side], preferred_element_type=jnp.float32)
                    + prm[side, layer, 5:6, :]
                )
                nhid[r, side * half : (side + 1) * half] = silu(pre).astype(jnp.bfloat16)
            update = jnp.dot(nhid[r, :], wrow[layer, 1], preferred_element_type=jnp.float32)
            average = jnp.mean(update, axis=1, keepdims=True)
            spread = jnp.mean(update * update, axis=1, keepdims=True) - average * average
            normed = (update - average) * lax.rsqrt(spread + norm_eps)
            normed = normed * gain_ref[layer : layer + 1, :] + nbias_ref[layer : layer + 1, :]
            result = (x.astype(jnp.float32) + normed).astype(jnp.bfloat16)
            if layer + 1 < layers:
                lat[r, :] = result
            else:
                out_ref[r, :] = result
            return 0

        lax.fori_loop(0, nblk, nodes, 0)

        halo_left.wait_send()
        halo_right.wait_send()

        def coarse_done(step, _):
            coarse_copy(step).wait_send()
            return 0

        lax.fori_loop(1, patches, coarse_done, 0)

    to_left.wait_send()
    to_right.wait_send()
    prm_out.wait_send()
    for layer in range(layers):
        for i in order:
            y_copy(layer, i).wait_send()
            f_copy(layer, i, core).wait_send()


def per_device(
    grid_latent,
    mesh_latent,
    grid_map,
    fine_senders,
    coarse_senders,
    fine_geom,
    coarse_geom,
    w_send,
    w_recv,
    w_geom,
    edge_bias,
    w_msg,
    msg_bias,
    w_node_h,
    w_node_a,
    node_bias,
    w_node_out,
    norm_gain,
    norm_bias,
):
    patches = lax.axis_size("ma")
    node_dev, features = mesh_latent.shape
    grid_dev = grid_latent.shape[0]
    co_dev, coarse_in = coarse_senders.shape
    fine_in, geo = fine_geom.shape[1], fine_geom.shape[2]
    layers, _, half = w_send.shape
    coarse = co_dev * patches
    co_edges = co_dev * coarse_in
    terms = 3
    ext = round_up(terms * slot_w * fine_in, 256)
    cext = 128

    ones = jnp.ones((node_dev, fine_in, 1), jnp.float32)
    rest = jnp.zeros((node_dev, fine_in, slot_w - geo - 1), jnp.float32)
    block = jnp.concatenate([fine_geom, ones, rest], axis=2).reshape(node_dev, fine_in * slot_w)
    fgeo = jnp.concatenate(
        [block] * terms + [jnp.zeros((node_dev, ext - terms * slot_w * fine_in), jnp.float32)],
        axis=1,
    )
    cg = jnp.transpose(coarse_geom, (1, 0, 2)).reshape(co_edges, geo)
    block = jnp.concatenate(
        [
            cg,
            jnp.ones((co_edges, 1), jnp.float32),
            jnp.zeros((co_edges, slot_w - geo - 1), jnp.float32),
        ],
        axis=1,
    )
    cgeo = jnp.concatenate(
        [block] * terms + [jnp.zeros((co_edges, cext - terms * slot_w), jnp.float32)], axis=1
    )
    cidx = jnp.transpose(coarse_senders).reshape(co_edges, 1)
    prm = jnp.concatenate(
        [
            w_geom,
            edge_bias[:, None, :],
            node_bias[:, None, :],
            jnp.zeros((layers, slot_w - geo - 2, half), jnp.float32),
        ],
        axis=1,
    )
    vmem = pl.BlockSpec(memory_space=pltpu.VMEM)
    hbm = pl.BlockSpec(memory_space=pl.ANY)
    dma = pltpu.SemaphoreType.DMA
    bf16, f32 = jnp.bfloat16, jnp.float32
    return pl.pallas_call(
        functools.partial(kernel, patches, terms),
        out_shape=jax.ShapeDtypeStruct((node_dev, features), bf16),
        in_specs=[hbm, vmem, vmem, vmem, vmem, vmem, vmem, hbm]
        + [hbm] * 6
        + [vmem] * 3,
        out_specs=vmem,
        scratch_shapes=[
            pltpu.VMEM((2 * grid_dev, features), bf16),
            pltpu.VMEM((node_dev, 2 * grid_dev), bf16),
            pltpu.VMEM((fine_in, node_dev, 2 * node_dev + ext), bf16),
            pltpu.VMEM((co_edges, coarse + cext), bf16),
            pltpu.VMEM((layers, 2 * node_dev + ext, features), bf16),
            pltpu.VMEM((layers, coarse + cext, features), bf16),
            pltpu.VMEM((node_dev, features), bf16),
            pltpu.VMEM((node_dev, features), bf16),
            pltpu.VMEM((node_dev, features), f32),
            pltpu.VMEM((node_dev, features), bf16),
            pltpu.VMEM((layers, 4, 2, features, half), bf16),
            pltpu.VMEM((layers, 2, 2 * half, features), bf16),
            pltpu.VMEM((2, layers, slot_w, half), f32),
            dma((layers + 1, 6)),
            dma((2,)),
            dma((2,)),
            dma((layers, 6)),
            dma((layers, 6)),
            dma((layers, 6)),
            dma((layers, 6)),
            dma((2,)),
            dma((layers, 2)),
            dma((layers, 2)),
            dma((layers, patches)),
            dma((layers, patches)),
        ],
        compiler_params=pltpu.CompilerParams(
            collective_id=0, has_side_effects=True, vmem_limit_bytes=60 * 1024 * 1024
        ),
        name="processor",
    )(
        grid_latent,
        mesh_latent,
        grid_map,
        fine_senders,
        cidx,
        fgeo,
        cgeo,
        prm,
        w_send,
        w_recv,
        w_node_h,
        w_node_a,
        w_msg,
        w_node_out,
        msg_bias,
        norm_gain,
        norm_bias,
    )


def solution(mesh):
    in_specs = (
        P("ma", None),
        P("ma", None),
        P("ma", None),
        P("ma", None),
        P("ma", None),
        P("ma", None, None),
        P("ma", None, None),
        P(None, None, "dev"),
        P(None, None, "dev"),
        P(None, None, "dev"),
        P(None, "dev"),
        P(None, "dev", None),
        P(),
        P(None, None, "dev"),
        P(None, None, "dev"),
        P(None, "dev"),
        P(None, "dev", None),
        P(),
        P(),
    )
    out_specs = P("ma", None)
    return jax.shard_map(
        per_device, mesh=mesh, in_specs=in_specs, out_specs=out_specs, check_vma=False
    )
```
